8 devices in a mesh: dp: 1 (over z), tp: 8 (over x, y, core).
Axes of the slice: x: 2, y: 2, z: 1, core: 2. Of those that a mesh axis runs over, the one named last changes fastest.
Arguments:
- x: bfloat16 [1024, 8192], P(('dp', 'tp'))
- w_gate: bfloat16 [8192, 28672], P(None, 'tp')
- w_up: bfloat16 [8192, 28672], P(None, 'tp')
- w_down: bfloat16 [28672, 8192], P('tp')
Outputs:
- output: bfloat16 [1024, 8192], P(('dp', 'tp'))
All inputs are finite; a program needn't handle non-finite values.
Results may differ from the reference program's by a relative error of at most 0.016.
Values are sent between devices in bfloat16 or wider.
A program may use at most 2 GiB of HBM per device.

```python
import jax
import jax.numpy as jnp

ROWS = 1024
D = 8192
FF = 28672


def setup_inputs(seed: int = 0, part: int = 0) -> dict:
    kx, kg, ku, kd = jax.random.split(jax.random.key(seed), 4)
    drawn = {
        "x": jax.random.normal(jax.random.fold_in(kx, part), (ROWS, D), jnp.float32),
        "w_gate": jax.random.normal(kg, (D, FF), jnp.float32) * D**-0.5,
        "w_up": jax.random.normal(ku, (D, FF), jnp.float32) * D**-0.5,
        "w_down": jax.random.normal(kd, (FF, D), jnp.float32) * FF**-0.5,
    }
    return {k: v.astype(jnp.bfloat16) for k, v in drawn.items()}


def reference(x, w_gate, w_up, w_down):
    gate = jnp.dot(x, w_gate, preferred_element_type=jnp.float32)
    up = jnp.dot(x, w_up, preferred_element_type=jnp.float32)
    hidden = (jax.nn.silu(gate) * up).astype(jnp.bfloat16)
    return jnp.dot(hidden, w_down, preferred_element_type=jnp.float32).astype(jnp.bfloat16)
```

```python
import functools

import jax
import jax.numpy as jnp
from jax import lax
from jax.experimental import pallas as pl
from jax.experimental.pallas import tpu as pltpu
from jax.sharding import PartitionSpec as P

F32, BF16 = jnp.float32, jnp.bfloat16
HALVES = 2
TILE = 256
WIDE = 512
CHUNKS = 8
EARLY = 7
SLOTS = 4
OWN = 7


def kernel(
    x_hbm, wg_hbm, wu_hbm, wd_hbm, y_hbm,
    xv, hid, ring, acc, send0, recv0, send1, recv1, send2, recv2, ost,
    wsem, xsem, osem, ag_s, ag_r, s0, r0, s1, r1, s2, r2, free0, free1, free2,
):
    rows = x_hbm.shape[0] // HALVES
    depth = x_hbm.shape[1]
    hidden = hid.shape[1]
    kc = depth // CHUNKS
    tiles = hidden // TILE
    late = tiles - EARLY
    pair = 2 * WIDE
    downs = depth // pair
    gathers = HALVES * CHUNKS
    sums = HALVES * downs
    group = 4 * rows

    me = lax.axis_index("tp")
    part = me + 1 - 2 * (me % 2)
    ynb = me + 2 - 4 * ((me // 2) % 2)
    xnb = (me + 4) % 8

    def rcopy(src, dst, ss, rs, dev):
        return pltpu.make_async_remote_copy(
            src_ref=src, dst_ref=dst, send_sem=ss, recv_sem=rs,
            device_id={"tp": dev}, device_id_type=pl.DeviceIdType.MESH,
        )

    def piece(q, block, lo, n):
        return xv.at[q // CHUNKS, pl.ds(block * rows + lo, n), pl.ds(pl.multiple_of((q % CHUNKS) * kc, kc), kc)]

    def ag(q, i, src, dst, dev):
        return rcopy(src, dst, ag_s.at[q, i], ag_r.at[q, i], dev)

    def ag_x(q):
        return ag(q, 0, piece(q, 0, 0, rows), piece(q, 2, 0, rows), xnb)

    def ag_y(q):
        return ag(q, 1, piece(q, 0, 0, rows), piece(q, 1, 0, rows), ynb)

    def ag_part(q, b):
        return ag(q, 2 + b, piece(q, b, 0, rows), piece(q, 4 + b, 0, rows), part)

    def ag_relay_y(q):
        return ag(q, 6, piece(q, 2, 0, rows // 2), piece(q, 3, 0, rows // 2), ynb)

    def ag_relay_x(q):
        return ag(q, 7, piece(q, 1, rows // 2, rows // 2), piece(q, 3, rows // 2, rows // 2), xnb)

    def gather_send(q):
        ag_x(q).start()
        ag_y(q).start()
        ag_part(q, 0).start()

    def gather_relay(q):
        ag_x(q).wait_recv()
        ag_relay_y(q).start()
        ag_y(q).wait_recv()
        ag_relay_x(q).start()
        ag_part(q, 2).start()
        ag_part(q, 1).start()

    def gather_diag(q):
        ag_relay_y(q).wait_recv()
        ag_relay_x(q).wait_recv()
        ag_part(q, 3).start()

    def gather_ready(q):
        for b in range(4):
            ag_part(q, b).wait_recv()

    def gather_sent(q):
        for c in (ag_x(q), ag_y(q), ag_relay_y(q), ag_relay_x(q), *(ag_part(q, b) for b in range(4))):
            c.wait_send()

    def w_early(t, slot):
        ks = pl.ds(pl.multiple_of(t * kc, kc), kc)
        out = []
        for n in range(EARLY):
            for j, w in enumerate((wg_hbm, wu_hbm)):
                dst = ring.at[slot, pl.ds(n * kc, kc), pl.ds(j * TILE, TILE)]
                out.append(pltpu.make_async_copy(w.at[ks, pl.ds(n * TILE, TILE)], dst, wsem.at[slot, 2 * n + j]))
        return out

    def w_full(t, slot):
        cols = pl.ds(pl.multiple_of(t * TILE, TILE), TILE)
        return [
            pltpu.make_async_copy(w.at[:, cols], ring.at[slot, :, pl.ds(j * TILE, TILE)], wsem.at[slot, j])
            for j, w in enumerate((wg_hbm, wu_hbm))
        ]

    def w_down(t, slot):
        return [
            pltpu.make_async_copy(
                wd_hbm.at[:, pl.ds(pl.multiple_of(t * pair + b * WIDE, WIDE), WIDE)],
                ring.at[slot, pl.ds(b * hidden, hidden), :],
                wsem.at[slot, b],
            )
            for b in range(2)
        ]

    def start(copies):
        for c in copies:
            c.start()

    def wait(copies):
        for c in copies:
            c.wait()

    def to_part(u):
        s = u % SLOTS
        return rcopy(send0.at[s], recv0.at[s], s0.at[s], r0.at[s], part)

    def to_first(u, b):
        s = u % SLOTS
        return rcopy(send1.at[s, b], recv1.at[s, b], s1.at[s, b], r1.at[s, b], (xnb, ynb)[b])

    def to_second(u, b):
        s = u % SLOTS
        return rcopy(send2.at[s, b], recv2.at[s, b], s2.at[s, b], r2.at[s, b], (ynb, xnb)[b])

    def out_copy(u):
        cols = pl.ds(pl.multiple_of((u % downs) * pair, pair), pair)
        return pltpu.make_async_copy(ost.at[u % 2], y_hbm.at[pl.ds((u // downs) * rows, rows), cols], osem.at[u % 2])

    def credit(sem, u, dev):
        @pl.when(u + SLOTS < sums)
        def _():
            pl.semaphore_signal(sem, inc=1, device_id={"tp": dev}, device_id_type=pl.DeviceIdType.MESH)

    def spend(sem, u):
        @pl.when(u >= SLOTS)
        def _():
            pl.semaphore_wait(sem, 1)

    def sum_first(u):
        s, o = u % SLOTS, u % OWN
        to_part(u).wait_recv()

        @pl.when(u >= SLOTS)
        def _():
            for b in range(2):
                to_first(u - SLOTS, b).wait_send()

        for b in range(2):
            cols = pl.ds(b * WIDE, WIDE)
            keep = (1, 2)[b]
            go = (2, 1)[b]
            for blk in (0, keep):
                at = pl.ds(b * group + blk * rows, rows)
                acc[o, at, :] += recv0[s, pl.ds(blk * rows, rows), cols].astype(F32)
            for i, blk in enumerate((go, 3)):
                at = pl.ds(b * group + blk * rows, rows)
                total = acc[o, at, :] + recv0[s, pl.ds(blk * rows, rows), cols].astype(F32)
                send1[s, b, pl.ds(i * rows, rows), :] = total.astype(BF16)
        credit(free0, u, part)
        for b in range(2):
            spend(free1.at[b], u)
            to_first(u, b).start()

    def sum_second(u):
        s, o = u % SLOTS, u % OWN
        for b in range(2):
            to_first(u, b).wait_recv()

        @pl.when(u >= SLOTS)
        def _():
            for b in range(2):
                to_second(u - SLOTS, b).wait_send()

        for b in range(2):
            keep = (1, 2)[b]
            mine = pl.ds(b * group, rows)
            acc[o, mine, :] += recv1[s, b, pl.ds(0, rows), :].astype(F32)
            total = acc[o, pl.ds(b * group + keep * rows, rows), :] + recv1[s, b, pl.ds(rows, rows), :].astype(F32)
            send2[s, b] = total.astype(BF16)
        for b in range(2):
            credit(free1.at[b], u, (xnb, ynb)[b])
            spend(free2.at[b], u)
            to_second(u, b).start()

    def sum_last(u):
        s, o = u % SLOTS, u % OWN
        for b in range(2):
            to_second(u, b).wait_recv()

        @pl.when(u >= 2)
        def _():
            out_copy(u - 2).wait()

        for b in range(2):
            total = acc[o, pl.ds(b * group, rows), :] + recv2[s, b].astype(F32)
            ost[u % 2, :, pl.ds(b * WIDE, WIDE)] = total.astype(BF16)
        for b in range(2):
            credit(free2.at[b], u, (ynb, xnb)[b])
        out_copy(u).start()

    def sums_at(v, lo):
        for lag, stage in ((1, sum_first), (3, sum_second), (5, sum_last)):
            u = v - lag

            @pl.when((u >= lo) & (u < lo + downs))
            def _():
                stage(u)

    def gated(gate, up):
        return (jax.nn.silu(gate) * up).astype(BF16)

    own = [
        pltpu.make_async_copy(x_hbm.at[pl.ds(h * rows, rows), :], xv.at[h, pl.ds(0, rows), :], xsem.at[h])
        for h in range(HALVES)
    ]
    start(own)
    start(w_early(0, 0))
    barrier = pltpu.get_barrier_semaphore()
    for dev in (part, ynb, xnb):
        pl.semaphore_signal(barrier, inc=1, device_id={"tp": dev}, device_id_type=pl.DeviceIdType.MESH)
    acc[...] = jnp.zeros_like(acc)
    pl.semaphore_wait(barrier, 3)
    wait(own)
    for q in range(2):
        gather_send(q)
    gather_relay(0)
    gather_send(2)
    gather_diag(0)

    def gather_at(g):
        @pl.when((g >= 1) & (g < gathers))
        def _():
            gather_diag(g)

        @pl.when(g + 1 < gathers)
        def _():
            gather_relay(g + 1)

        @pl.when(g + 3 < gathers)
        def _():
            gather_send(g + 3)

    def early_trip(t, _):
        slot = t % 2
        gather_at(t)
        wait(w_early(t, slot))

        @pl.when(t + 1 < CHUNKS)
        def _():
            start(w_early(t + 1, 1 - slot))

        @pl.when(t + 1 == CHUNKS)
        def _():
            start(w_full(EARLY, 1 - slot))

        gather_ready(t)
        for n in range(EARLY):
            acc[n] += jnp.dot(
                xv[0, :, pl.ds(pl.multiple_of(t * kc, kc), kc)],
                ring[slot, n * kc : (n + 1) * kc, :],
                preferred_element_type=F32,
            )
        return 0

    lax.fori_loop(0, CHUNKS, early_trip, 0)

    def full_tile(h, t, slot):
        r = jnp.dot(xv[h], ring[slot], preferred_element_type=F32)
        hid[:, pl.ds(pl.multiple_of(t * TILE, TILE), TILE)] = gated(r[:, :TILE], r[:, TILE:])

    base = CHUNKS

    def late_trip(t, _):
        slot = (base + t) % 2
        gather_at(CHUNKS + t)
        wait(w_full(EARLY + t, slot))

        @pl.when(t + 1 < late)
        def _():
            start(w_full(EARLY + t + 1, 1 - slot))

        @pl.when(t + 1 == late)
        def _():
            start(w_down(0, 1 - slot))

        full_tile(0, EARLY + t, slot)
        a = acc[t]
        hid[:, pl.ds(pl.multiple_of(t * TILE, TILE), TILE)] = gated(a[:, :TILE], a[:, TILE:])
        return 0

    lax.fori_loop(0, late, late_trip, 0)
    base += late
    for q in range(base, gathers):
        gather_diag(q)

    def down_loop(h, base, lo):
        def trip(t, _):
            slot = (base + t) % 2
            u = lo + t
            sums_at(u, lo)
            wait(w_down(t, slot))

            @pl.when(t + 1 < downs)
            def _():
                start(w_down(t + 1, 1 - slot))

            if h + 1 < HALVES:

                @pl.when(t + 1 == downs)
                def _():
                    start(w_full(0, 1 - slot))

            @pl.when(u >= SLOTS)
            def _():
                to_part(u - SLOTS).wait_send()

            s, o = u % SLOTS, u % OWN
            for b in range(2):
                r = jnp.dot(hid[...], ring[slot, b * hidden : (b + 1) * hidden, :], preferred_element_type=F32)
                acc[o, pl.ds(b * group, group), :] = r[:group]
                send0[s, :, b * WIDE : (b + 1) * WIDE] = r[group:].astype(BF16)
            spend(free0, u)
            to_part(u).start()
            return 0

        lax.fori_loop(0, downs, trip, 0)

    down_loop(0, base, 0)
    base += downs

    def drain(q, _):
        gather_ready(q)
        return 0

    lax.fori_loop(CHUNKS, gathers, drain, 0)

    def full_trip(t, _):
        slot = (base + t) % 2
        sums_at(downs + t, 0)
        wait(w_full(t, slot))

        @pl.when(t + 1 < tiles)
        def _():
            start(w_full(t + 1, 1 - slot))

        @pl.when(t + 1 == tiles)
        def _():
            start(w_down(0, 1 - slot))

        full_tile(1, t, slot)
        return 0

    lax.fori_loop(0, tiles, full_trip, 0)
    down_loop(1, base + tiles, downs)

    def tail(v, _):
        sums_at(v, downs)
        return 0

    lax.fori_loop(sums, sums + 5, tail, 0)

    def sent(q, _):
        gather_sent(q)
        return 0

    lax.fori_loop(0, gathers, sent, 0)

    def last(u, _):
        to_part(u).wait_send()
        for b in range(2):
            to_first(u, b).wait_send()
            to_second(u, b).wait_send()
        return 0

    lax.fori_loop(sums - SLOTS, sums, last, 0)
    for u in (sums - 2, sums - 1):
        out_copy(u).wait()


def solution(mesh):
    def step(x, w_gate, w_up, w_down):
        n = mesh.shape["tp"]
        rows, depth = x.shape
        hidden = w_gate.shape[1]
        m = n * rows // HALVES
        r = rows // HALVES
        gathers = HALVES * CHUNKS
        dma = pltpu.SemaphoreType.DMA
        return pl.pallas_call(
            kernel,
            out_shape=jax.ShapeDtypeStruct((rows, depth), BF16),
            in_specs=[pl.BlockSpec(memory_space=pltpu.HBM)] * 4,
            out_specs=pl.BlockSpec(memory_space=pltpu.HBM),
            scratch_shapes=[
                pltpu.VMEM((HALVES, m, depth), BF16),
                pltpu.VMEM((m, hidden), BF16),
                pltpu.VMEM((2, depth, 2 * TILE), BF16),
                pltpu.VMEM((EARLY, m, 2 * TILE), F32),
                pltpu.VMEM((SLOTS, 4 * r, 2 * WIDE), BF16),
                pltpu.VMEM((SLOTS, 4 * r, 2 * WIDE), BF16),
                pltpu.VMEM((SLOTS, 2, 2 * r, WIDE), BF16),
                pltpu.VMEM((SLOTS, 2, 2 * r, WIDE), BF16),
                pltpu.VMEM((SLOTS, 2, r, WIDE), BF16),
                pltpu.VMEM((SLOTS, 2, r, WIDE), BF16),
                pltpu.VMEM((2, r, 2 * WIDE), BF16),
                dma((2, 2 * EARLY)),
                dma((HALVES,)),
                dma((2,)),
                dma((gathers, 8)),
                dma((gathers, 8)),
                dma((SLOTS,)),
                dma((SLOTS,)),
                dma((SLOTS, 2)),
                dma((SLOTS, 2)),
                dma((SLOTS, 2)),
                dma((SLOTS, 2)),
                pltpu.SemaphoreType.REGULAR,
                pltpu.SemaphoreType.REGULAR((2,)),
                pltpu.SemaphoreType.REGULAR((2,)),
            ],
            compiler_params=pltpu.CompilerParams(
                collective_id=0, has_side_effects=True, vmem_limit_bytes=67043328
            ),
        )(x, w_gate, w_up, w_down)

    return jax.shard_map(
        step,
        mesh=mesh,
        in_specs=(P(("dp", "tp"), None), P(None, "tp"), P(None, "tp"), P("tp", None)),
        out_specs=P(("dp", "tp"), None),
        check_vma=False,
    )
```

```python
import functools

import jax
import jax.numpy as jnp
from jax import lax
from jax.experimental import pallas as pl
from jax.experimental.pallas import tpu as pltpu
from jax.sharding import PartitionSpec as P

F32, BF16 = jnp.float32, jnp.bfloat16
HALVES = 2
TILE = 256
WIDE = 512
CHUNKS = (16, 8)
SLOTS = 5
OWN = 12


def kernel(
    x_hbm, wg_hbm, wu_hbm, wd_hbm, y_hbm,
    xv, hid, ring, acc, send0, recv0, send1, recv1, send2, recv2, ost,
    wsem, xsem, osem, ag_s, ag_r, s0, r0, s1, r1, s2, r2, free0, free1, free2,
):
    rows = x_hbm.shape[0] // HALVES
    depth = x_hbm.shape[1]
    hidden = hid.shape[1]
    kcs = [depth // n for n in CHUNKS]
    tiles = hidden // TILE
    blocks = hidden // WIDE
    pair = 2 * WIDE
    downs = depth // pair
    sums = HALVES * downs
    group = 4 * rows

    me = lax.axis_index("tp")
    part = me + 1 - 2 * (me % 2)
    ynb = me + 2 - 4 * ((me // 2) % 2)
    xnb = (me + 4) % 8

    def rcopy(src, dst, ss, rs, dev):
        return pltpu.make_async_remote_copy(
            src_ref=src, dst_ref=dst, send_sem=ss, recv_sem=rs,
            device_id={"tp": dev}, device_id_type=pl.DeviceIdType.MESH,
        )

    def piece(h, c, block, lo, n):
        return xv.at[h, pl.ds(block * rows + lo, n), pl.ds(pl.multiple_of(c * kcs[h], kcs[h]), kcs[h])]

    def ag(h, c, i, src, dst, dev):
        q = h * CHUNKS[0] + c
        return rcopy(piece(h, c, *src), piece(h, c, *dst), ag_s.at[q, i], ag_r.at[q, i], dev)

    def ag_x(h, c):
        return ag(h, c, 0, (0, 0, rows), (2, 0, rows), xnb)

    def ag_y(h, c):
        return ag(h, c, 1, (0, 0, rows), (1, 0, rows), ynb)

    def ag_part(h, c, b):
        return ag(h, c, 2 + b, (b, 0, rows), (4 + b, 0, rows), part)

    def ag_relay_y(h, c):
        return ag(h, c, 6, (2, 0, rows // 2), (3, 0, rows // 2), ynb)

    def ag_relay_x(h, c):
        return ag(h, c, 7, (1, rows // 2, rows // 2), (3, rows // 2, rows // 2), xnb)

    def gather_send(h, c):
        ag_x(h, c).start()
        ag_y(h, c).start()
        ag_part(h, c, 0).start()

    def gather_relay(h, c):
        ag_x(h, c).wait_recv()
        ag_relay_y(h, c).start()
        ag_y(h, c).wait_recv()
        ag_relay_x(h, c).start()
        ag_part(h, c, 2).start()
        ag_part(h, c, 1).start()

    def gather_diag(h, c):
        ag_relay_y(h, c).wait_recv()
        ag_relay_x(h, c).wait_recv()
        ag_part(h, c, 3).start()

    def gather_ready(h, c):
        for b in range(4):
            ag_part(h, c, b).wait_recv()

    def gather_sent(h, c):
        parts = [ag_part(h, c, b) for b in range(4)]
        for copy in (ag_x(h, c), ag_y(h, c), ag_relay_y(h, c), ag_relay_x(h, c), *parts):
            copy.wait_send()

    def w_chunk(t, slot):
        ks = pl.ds(pl.multiple_of(t * kcs[0], kcs[0]), kcs[0])
        return [
            pltpu.make_async_copy(
                w.at[ks, pl.ds(n * WIDE, WIDE)],
                ring.at[slot, pl.ds((j * blocks + n) * kcs[0], kcs[0]), :],
                wsem.at[slot],
            )
            for j, w in enumerate((wg_hbm, wu_hbm))
            for n in range(blocks)
        ]

    def w_full(t, slot):
        cols = pl.ds(pl.multiple_of(t * TILE, TILE), TILE)
        return [
            pltpu.make_async_copy(w.at[:, cols], ring.at[slot, :, pl.ds(j * TILE, TILE)], wsem.at[slot])
            for j, w in enumerate((wg_hbm, wu_hbm))
        ]

    def w_down(t, slot):
        return [
            pltpu.make_async_copy(
                wd_hbm.at[:, pl.ds(pl.multiple_of(t * pair + b * WIDE, WIDE), WIDE)],
                ring.at[slot, pl.ds(b * hidden, hidden), :],
                wsem.at[slot],
            )
            for b in range(2)
        ]

    def start(copies):
        for c in copies:
            c.start()

    def wait(copies):
        for c in copies:
            c.wait()

    def arrived(slot, n):
        block = ring.at[slot, pl.ds(0, n), :]
        pltpu.make_async_copy(block, block, wsem.at[slot]).wait()

    def to_part(u, b):
        s = u % SLOTS
        return rcopy(send0.at[s, b], recv0.at[s, b], s0.at[s, b], r0.at[s, b], part)

    def to_first(u, b):
        s = u % SLOTS
        return rcopy(send1.at[s, b], recv1.at[s, b], s1.at[s, b], r1.at[s, b], (xnb, ynb)[b])

    def to_second(u, b):
        s = u % SLOTS
        return rcopy(send2.at[s, b], recv2.at[s, b], s2.at[s, b], r2.at[s, b], (ynb, xnb)[b])

    def out_copy(u, b):
        cols = pl.ds(pl.multiple_of((u % downs) * pair + b * WIDE, WIDE), WIDE)
        at = pl.ds((u // downs) * rows, rows)
        return pltpu.make_async_copy(ost.at[u % 2, b], y_hbm.at[at, cols], osem.at[u % 2, b])

    def when(cond, f, *args):
        @pl.when(cond)
        def _():
            f(*args)

    def credit(sem, u, dev):
        @pl.when(u + SLOTS < sums)
        def _():
            pl.semaphore_signal(sem, inc=1, device_id={"tp": dev}, device_id_type=pl.DeviceIdType.MESH)

    def spend(sem, u):
        @pl.when(u >= SLOTS)
        def _():
            pl.semaphore_wait(sem, 1)

    def sum_first(u, b):
        s, o = u % SLOTS, u % OWN
        to_part(u, b).wait_recv()
        when(u >= SLOTS, lambda: to_first(u - SLOTS, b).wait_send())
        for blk in (0, (1, 2)[b]):
            acc[o, pl.ds(b * group + blk * rows, rows), :] += recv0[s, b, pl.ds(blk * rows, rows), :].astype(F32)
        for i, blk in enumerate(((2, 1)[b], 3)):
            total = acc[o, pl.ds(b * group + blk * rows, rows), :] + recv0[s, b, pl.ds(blk * rows, rows), :].astype(F32)
            send1[s, b, pl.ds(i * rows, rows), :] = total.astype(BF16)
        credit(free0.at[b], u, part)
        spend(free1.at[b], u)
        to_first(u, b).start()

    def sum_second(u, b):
        s, o = u % SLOTS, u % OWN
        to_first(u, b).wait_recv()
        when(u >= SLOTS, lambda: to_second(u - SLOTS, b).wait_send())
        keep = (1, 2)[b]
        acc[o, pl.ds(b * group, rows), :] += recv1[s, b, pl.ds(0, rows), :].astype(F32)
        total = acc[o, pl.ds(b * group + keep * rows, rows), :] + recv1[s, b, pl.ds(rows, rows), :].astype(F32)
        send2[s, b] = total.astype(BF16)
        credit(free1.at[b], u, (xnb, ynb)[b])
        spend(free2.at[b], u)
        to_second(u, b).start()

    def sum_last(u, b):
        s, o = u % SLOTS, u % OWN
        to_second(u, b).wait_recv()
        when(u >= 2, lambda: out_copy(u - 2, b).wait())
        total = acc[o, pl.ds(b * group, rows), :] + recv2[s, b].astype(F32)
        ost[u % 2, b] = total.astype(BF16)
        credit(free2.at[b], u, (ynb, xnb)[b])
        out_copy(u, b).start()

    def stages(v, lo, due):
        for stage, lag, b in due:
            u = v - lag
            when((u >= lo) & (u < lo + downs), stage, u, b)

    once = [(f, lag, b) for f, lag in ((sum_second, 7), (sum_first, 4), (sum_last, 10)) for b in range(2)]
    at_start = [(sum_second, 3, 1), (sum_first, 1, 0), (sum_last, 4, 1)]
    at_middle = [(sum_second, 2, 0), (sum_first, 1, 1), (sum_last, 3, 0)]

    def gated(gate, up):
        return (jax.nn.silu(gate) * up).astype(BF16)

    own = [
        pltpu.make_async_copy(x_hbm.at[pl.ds(h * rows, rows), cols], xv.at[h, pl.ds(0, rows), cols], xsem.at[i])
        for i, (h, cols) in enumerate(
            ((0, pl.ds(0, kcs[0])), (0, pl.ds(kcs[0], depth - kcs[0])), (1, pl.ds(0, depth)))
        )
    ]
    start(own[:1])
    barrier = pltpu.get_barrier_semaphore()
    for dev in (part, ynb, xnb):
        pl.semaphore_signal(barrier, inc=1, device_id={"tp": dev}, device_id_type=pl.DeviceIdType.MESH)
    start(own[1:])
    start(w_chunk(0, 0))
    wait(own[:1])
    pl.semaphore_wait(barrier, 3)
    gather_send(0, 0)
    wait(own[1:])
    gather_relay(0, 0)
    gather_send(0, 1)
    gather_send(0, 2)
    gather_diag(0, 0)
    gather_relay(0, 1)
    gather_send(0, 3)

    def chunk_comm(t):
        when(t + 1 < CHUNKS[0], gather_diag, 0, t + 1)
        when(t + 2 < CHUNKS[0], gather_relay, 0, t + 2)
        when(t + 4 < CHUNKS[0], gather_send, 0, t + 4)
        when(t % 3 == 1, gather_send, 1, t // 3)
        when((t % 3 == 0) & (t >= 3), gather_relay, 1, (t - 3) // 3)
        when((t % 3 == 2) & (t >= 5), gather_diag, 1, (t - 5) // 3)

    def chunk_product(t, slot, n):
        return jnp.dot(
            xv[0, :, pl.ds(pl.multiple_of(t * kcs[0], kcs[0]), kcs[0])],
            ring[slot, n * kcs[0] : (n + 1) * kcs[0], :],
            preferred_element_type=F32,
        )

    def chunk_trip(t, _):
        slot = t % 2
        chunk_comm(t)
        arrived(slot, 2 * blocks * kcs[0])
        start(w_chunk(t + 1, 1 - slot))
        gather_ready(0, t)
        for n in range(2 * blocks):
            acc[n] += chunk_product(t, slot, n)
        return 0

    final = CHUNKS[0] - 1
    arrived(0, 2 * blocks * kcs[0])
    start(w_chunk(1, 1))
    gather_ready(0, 0)
    for n in range(blocks):
        acc[n] = chunk_product(0, 0, n)
    chunk_comm(0)
    for n in range(blocks, 2 * blocks):
        acc[n] = chunk_product(0, 0, n)
    lax.fori_loop(1, final, chunk_trip, 0)
    chunk_comm(final)
    arrived(final % 2, 2 * blocks * kcs[0])
    start(w_down(0, 1 - final % 2))
    gather_ready(0, final)
    for n in range(blocks):
        gate = acc[n] + chunk_product(final, final % 2, n)
        up = acc[blocks + n] + chunk_product(final, final % 2, blocks + n)
        hid[:, n * WIDE : (n + 1) * WIDE] = gated(gate, up)
    base = CHUNKS[0]

    def full_tile(h, t, slot):
        r = jnp.dot(xv[h], ring[slot], preferred_element_type=F32)
        hid[:, pl.ds(pl.multiple_of(t * TILE, TILE), TILE)] = gated(r[:, :TILE], r[:, TILE:])

    def down_loop(h, base, lo):
        def trip(t, _):
            slot = (base + t) % 2
            u = lo + t
            stages(u, lo, at_start if h else once)
            if h == 0:
                when(t == 1, gather_diag, 1, 4)
                when(t < 3, gather_send, 1, 5 + t)
                when((t >= 2) & (t < 5), gather_relay, 1, 3 + t)
                when((t >= 4) & (t < 7), gather_diag, 1, 1 + t)
            arrived(slot, 2 * hidden)

            @pl.when(t + 1 < downs)
            def _():
                start(w_down(t + 1, 1 - slot))

            if h + 1 < HALVES:

                @pl.when(t + 1 == downs)
                def _():
                    start(w_full(0, 1 - slot))

            @pl.when(u >= SLOTS)
            def _():
                for b in range(2):
                    to_part(u - SLOTS, b).wait_send()
                    spend(free0.at[b], u)

            s, o = u % SLOTS, u % OWN
            for b in range(2):
                r = jnp.dot(hid[...], ring[slot, b * hidden : (b + 1) * hidden, :], preferred_element_type=F32)
                acc[o, pl.ds(b * group, group), :] = r[:group]
                send0[s, b] = r[group:].astype(BF16)
                if h:
                    to_part(u, b).start()
                    if b == 0:
                        stages(u, lo, at_middle)
            if not h:
                for b in range(2):
                    to_part(u, b).start()
            return 0

        lax.fori_loop(0, downs, trip, 0)

    down_loop(0, base, 0)
    base += downs

    def drain(c, _):
        gather_ready(1, c)
        return 0

    lax.fori_loop(0, CHUNKS[1], drain, 0)

    def full_trip(t, _):
        slot = (base + t) % 2
        stages(downs + t, 0, once)
        arrived(slot, depth)

        @pl.when(t + 1 < tiles)
        def _():
            start(w_full(t + 1, 1 - slot))

        @pl.when(t + 1 == tiles)
        def _():
            start(w_down(0, 1 - slot))

        full_tile(1, t, slot)
        return 0

    lax.fori_loop(0, tiles, full_trip, 0)
    down_loop(1, base + tiles, downs)

    def tail(v, _):
        stages(v, downs, at_start)
        stages(v, downs, at_middle)
        return 0

    lax.fori_loop(sums, sums + 4, tail, 0)

    for h in range(HALVES):

        def sent(c, _):
            gather_sent(h, c)
            return 0

        lax.fori_loop(0, CHUNKS[h], sent, 0)

    def last(u, _):
        for b in range(2):
            to_part(u, b).wait_send()
            to_first(u, b).wait_send()
            to_second(u, b).wait_send()
        return 0

    lax.fori_loop(sums - SLOTS, sums, last, 0)
    for u in (sums - 2, sums - 1):
        for b in range(2):
            out_copy(u, b).wait()


def solution(mesh):
    def step(x, w_gate, w_up, w_down):
        n = mesh.shape["tp"]
        rows, depth = x.shape
        hidden = w_gate.shape[1]
        m = n * rows // HALVES
        r = rows // HALVES
        gathers = sum(CHUNKS)
        blocks = 2 * hidden // WIDE
        dma = pltpu.SemaphoreType.DMA
        return pl.pallas_call(
            kernel,
            out_shape=jax.ShapeDtypeStruct((rows, depth), BF16),
            in_specs=[pl.BlockSpec(memory_space=pltpu.HBM)] * 4,
            out_specs=pl.BlockSpec(memory_space=pltpu.HBM),
            scratch_shapes=[
                pltpu.VMEM((HALVES, m, depth), BF16),
                pltpu.VMEM((m, hidden), BF16),
                pltpu.VMEM((2, depth, 2 * TILE), BF16),
                pltpu.VMEM((blocks, m, WIDE), F32),
                pltpu.VMEM((SLOTS, 2, 4 * r, WIDE), BF16),
                pltpu.VMEM((SLOTS, 2, 4 * r, WIDE), BF16),
                pltpu.VMEM((SLOTS, 2, 2 * r, WIDE), BF16),
                pltpu.VMEM((SLOTS, 2, 2 * r, WIDE), BF16),
                pltpu.VMEM((SLOTS, 2, r, WIDE), BF16),
                pltpu.VMEM((SLOTS, 2, r, WIDE), BF16),
                pltpu.VMEM((2, 2, r, WIDE), BF16),
                dma((2,)),
                dma((3,)),
                dma((2, 2)),
                dma((gathers, 8)),
                dma((gathers, 8)),
                dma((SLOTS, 2)),
                dma((SLOTS, 2)),
                dma((SLOTS, 2)),
                dma((SLOTS, 2)),
                dma((SLOTS, 2)),
                dma((SLOTS, 2)),
                pltpu.SemaphoreType.REGULAR((2,)),
                pltpu.SemaphoreType.REGULAR((2,)),
                pltpu.SemaphoreType.REGULAR((2,)),
            ],
            compiler_params=pltpu.CompilerParams(
                collective_id=0, has_side_effects=True, vmem_limit_bytes=67043328
            ),
        )(x, w_gate, w_up, w_down)

    return jax.shard_map(
        step,
        mesh=mesh,
        in_specs=(P(("dp", "tp"), None), P(None, "tp"), P(None, "tp"), P("tp", None)),
        out_specs=P(("dp", "tp"), None),
        check_vma=False,
    )
```

```python
import functools

import jax
import jax.numpy as jnp
from jax import lax
from jax.experimental import pallas as pl
from jax.experimental.pallas import tpu as pltpu
from jax.sharding import PartitionSpec as P

F32, BF16 = jnp.float32, jnp.bfloat16
HALVES = 2
TILE = 256
WIDE = 512
NARROW = WIDE // 2
CHUNKS = (16, 8)
MOVES = 8
SLOTS = 5
OWN = 12


def kernel(
    x_hbm, wg_hbm, wu_hbm, wd_hbm, y_hbm,
    xv, hid, ring, acc, send0, recv0, send1, recv1, send2, recv2, ost,
    wsem, xsem, osem, ag_s, ag_r, s0, r0, s1, r1, s2, r2, free0, free1, free2,
):
    rows = x_hbm.shape[0] // HALVES
    depth = x_hbm.shape[1]
    hidden = hid.shape[1]
    kcs = [depth // n for n in CHUNKS]
    tiles = hidden // TILE
    blocks = hidden // WIDE
    pair = 2 * WIDE
    downs = depth // pair
    sums = HALVES * downs
    group = 4 * rows

    me = lax.axis_index("tp")
    part = me + 1 - 2 * (me % 2)
    ynb = me + 2 - 4 * ((me // 2) % 2)
    xnb = (me + 4) % 8

    def rcopy(src, dst, ss, rs, dev):
        return pltpu.make_async_remote_copy(
            src_ref=src, dst_ref=dst, send_sem=ss, recv_sem=rs,
            device_id={"tp": dev}, device_id_type=pl.DeviceIdType.MESH,
        )

    def piece(h, c, block, lo, n):
        return xv.at[h, pl.ds(block * rows + lo, n), pl.ds(pl.multiple_of(c * kcs[h], kcs[h]), kcs[h])]

    def ag(h, c, i, src, dst, dev):
        q = h * CHUNKS[0] + c
        return rcopy(piece(h, c, *src), piece(h, c, *dst), ag_s.at[q, i], ag_r.at[q, i], dev)

    def ag_x(h, c):
        return ag(h, c, 0, (0, 0, rows), (2, 0, rows), xnb)

    def ag_y(h, c):
        return ag(h, c, 1, (0, 0, rows), (1, 0, rows), ynb)

    def ag_part(h, c, b):
        return ag(h, c, 2 + b, (b, 0, rows), (4 + b, 0, rows), part)

    def ag_relay_y(h, c):
        return ag(h, c, 6, (2, 0, rows // 2), (3, 0, rows // 2), ynb)

    def ag_relay_x(h, c):
        return ag(h, c, 7, (1, rows // 2, rows // 2), (3, rows // 2, rows // 2), xnb)

    def gather_send(h, c):
        ag_x(h, c).start()
        ag_y(h, c).start()
        ag_part(h, c, 0).start()

    def gather_relay(h, c):
        ag_x(h, c).wait_recv()
        ag_relay_y(h, c).start()
        ag_y(h, c).wait_recv()
        ag_relay_x(h, c).start()
        ag_part(h, c, 2).start()
        ag_part(h, c, 1).start()

    def gather_diag(h, c):
        ag_relay_y(h, c).wait_recv()
        ag_relay_x(h, c).wait_recv()
        ag_part(h, c, 3).start()

    def gather_ready(h, c):
        for b in range(4):
            ag_part(h, c, b).wait_recv()

    def gather_sent(h, c):
        parts = [ag_part(h, c, b) for b in range(4)]
        for copy in (ag_x(h, c), ag_y(h, c), ag_relay_y(h, c), ag_relay_x(h, c), *parts):
            copy.wait_send()

    def w_chunk(t, slot):
        ks = pl.ds(pl.multiple_of(t * kcs[0], kcs[0]), kcs[0])
        return [
            pltpu.make_async_copy(
                w.at[ks, pl.ds(n * WIDE, WIDE)],
                ring.at[slot, pl.ds((j * blocks + n) * kcs[0], kcs[0]), :],
                wsem.at[slot],
            )
            for j, w in enumerate((wg_hbm, wu_hbm))
            for n in range(blocks)
        ]

    def w_full(t, slot):
        cols = pl.ds(pl.multiple_of(t * TILE, TILE), TILE)
        return [
            pltpu.make_async_copy(w.at[:, cols], ring.at[slot, :, pl.ds(j * TILE, TILE)], wsem.at[slot])
            for j, w in enumerate((wg_hbm, wu_hbm))
        ]

    def w_down(t, slot):
        return [
            pltpu.make_async_copy(
                wd_hbm.at[:, pl.ds(pl.multiple_of(t * pair + b * WIDE, WIDE), WIDE)],
                ring.at[slot, pl.ds(b * hidden, hidden), :],
                wsem.at[slot],
            )
            for b in range(2)
        ]

    def start(copies):
        for c in copies:
            c.start()

    def wait(copies):
        for c in copies:
            c.wait()

    def arrived(slot, n):
        block = ring.at[slot, pl.ds(0, n), :]
        pltpu.make_async_copy(block, block, wsem.at[slot]).wait()

    def to_part(u, b):
        s = u % SLOTS
        return rcopy(send0.at[s, b], recv0.at[s, b], s0.at[s, b], r0.at[s, b], part)

    def to_first(u, b, c):
        s = u % SLOTS
        return rcopy(send1.at[s, b, c], recv1.at[s, b, c], s1.at[s, b, c], r1.at[s, b, c], (xnb, ynb)[c])

    def to_second(u, b, c):
        s = u % SLOTS
        return rcopy(send2.at[s, b, c], recv2.at[s, b, c], s2.at[s, b, c], r2.at[s, b, c], (ynb, xnb)[c])

    def out_copy(u, b):
        cols = pl.ds(pl.multiple_of((u % downs) * pair + b * WIDE, WIDE), WIDE)
        at = pl.ds((u // downs) * rows, rows)
        return pltpu.make_async_copy(ost.at[u % 2, b], y_hbm.at[at, cols], osem.at[u % 2, b])

    def when(cond, f, *args):
        @pl.when(cond)
        def _():
            f(*args)

    def credit(sem, u, dev):
        @pl.when(u + SLOTS < sums)
        def _():
            pl.semaphore_signal(sem, inc=1, device_id={"tp": dev}, device_id_type=pl.DeviceIdType.MESH)

    def spend(sem, u):
        @pl.when(u >= SLOTS)
        def _():
            pl.semaphore_wait(sem, 1)

    def own_term(u, b, c, block):
        return acc.at[u % OWN, pl.ds(b * group + block * rows, rows), pl.ds(c * NARROW, NARROW)]

    def sum_first(u, b):
        s = u % SLOTS
        to_part(u, b).wait_recv()

        @pl.when(u >= SLOTS)
        def _():
            for c in range(2):
                to_first(u - SLOTS, b, c).wait_send()

        for c in range(2):

            def other(block):
                return recv0[s, b, pl.ds(block * rows, rows), pl.ds(c * NARROW, NARROW)].astype(F32)

            for i, block in enumerate(((2, 1)[c], 3)):
                total = own_term(u, b, c, block)[...] + other(block)
                send1[s, b, c, pl.ds(i * rows, rows), :] = total.astype(BF16)
            for block in (0, (1, 2)[c]):
                mine = own_term(u, b, c, block)
                mine[...] = mine[...] + other(block)
        for c in range(2):
            spend(free1.at[b, c], u)
            to_first(u, b, c).start()
        credit(free0.at[b], u, part)

    def sum_second(u, b):
        s = u % SLOTS
        for c in range(2):
            to_first(u, b, c).wait_recv()

        @pl.when(u >= SLOTS)
        def _():
            for c in range(2):
                to_second(u - SLOTS, b, c).wait_send()

        for c in range(2):
            total = own_term(u, b, c, (1, 2)[c])[...] + recv1[s, b, c, pl.ds(rows, rows), :].astype(F32)
            send2[s, b, c] = total.astype(BF16)
            mine = own_term(u, b, c, 0)
            mine[...] = mine[...] + recv1[s, b, c, pl.ds(0, rows), :].astype(F32)
        for c in range(2):
            spend(free2.at[b, c], u)
            to_second(u, b, c).start()
        for c in range(2):
            credit(free1.at[b, c], u, (xnb, ynb)[c])

    def sum_last(u, b):
        s = u % SLOTS
        for c in range(2):
            to_second(u, b, c).wait_recv()
        when(u >= 2, lambda: out_copy(u - 2, b).wait())
        for c in range(2):
            total = own_term(u, b, c, 0)[...] + recv2[s, b, c].astype(F32)
            ost[u % 2, b, :, pl.ds(c * NARROW, NARROW)] = total.astype(BF16)
        out_copy(u, b).start()
        for c in range(2):
            credit(free2.at[b, c], u, (ynb, xnb)[c])

    def stages(v, lo, due):
        for stage, lag, b in due:
            u = v - lag
            when((u >= lo) & (u < lo + downs), stage, u, b)

    once = [(f, lag, b) for f, lag in ((sum_second, 7), (sum_first, 4), (sum_last, 10)) for b in range(2)]
    at_start, at_middle = ([(sum_first, 1, b), (sum_second, 2, b), (sum_last, 3, b)] for b in range(2))

    def gated(gate, up):
        return (jax.nn.silu(gate) * up).astype(BF16)

    own = [
        pltpu.make_async_copy(x_hbm.at[pl.ds(h * rows, rows), cols], xv.at[h, pl.ds(0, rows), cols], xsem.at[i])
        for i, (h, cols) in enumerate(
            ((0, pl.ds(0, kcs[0])), (0, pl.ds(kcs[0], depth - kcs[0])), (1, pl.ds(0, depth)))
        )
    ]
    start(own[:1])
    barrier = pltpu.get_barrier_semaphore()
    for dev in (part, ynb, xnb):
        pl.semaphore_signal(barrier, inc=1, device_id={"tp": dev}, device_id_type=pl.DeviceIdType.MESH)
    start(own[1:])
    start(w_chunk(0, 0))
    wait(own[:1])
    pl.semaphore_wait(barrier, 3)
    gather_send(0, 0)
    wait(own[1:])
    gather_relay(0, 0)
    gather_send(0, 1)
    gather_send(0, 2)
    gather_diag(0, 0)
    gather_relay(0, 1)
    gather_send(0, 3)

    def chunk_comm(t):
        when(t + 1 < CHUNKS[0], gather_diag, 0, t + 1)
        when(t + 2 < CHUNKS[0], gather_relay, 0, t + 2)
        when(t + 4 < CHUNKS[0], gather_send, 0, t + 4)
        when(t % 3 == 1, gather_send, 1, t // 3)
        when((t % 3 == 0) & (t >= 3), gather_relay, 1, (t - 3) // 3)
        when((t % 3 == 2) & (t >= 5), gather_diag, 1, (t - 5) // 3)

    def chunk_product(t, slot, n):
        return jnp.dot(
            xv[0, :, pl.ds(pl.multiple_of(t * kcs[0], kcs[0]), kcs[0])],
            ring[slot, n * kcs[0] : (n + 1) * kcs[0], :],
            preferred_element_type=F32,
        )

    def chunk_trip(t, _):
        slot = t % 2
        chunk_comm(t)
        arrived(slot, 2 * blocks * kcs[0])
        start(w_chunk(t + 1, 1 - slot))
        gather_ready(0, t)
        for n in range(2 * blocks):
            acc[n] += chunk_product(t, slot, n)
        return 0

    final = CHUNKS[0] - 1
    arrived(0, 2 * blocks * kcs[0])
    start(w_chunk(1, 1))
    gather_ready(0, 0)
    for n in range(blocks):
        acc[n] = chunk_product(0, 0, n)
    chunk_comm(0)
    for n in range(blocks, 2 * blocks):
        acc[n] = chunk_product(0, 0, n)
    lax.fori_loop(1, final, chunk_trip, 0)
    chunk_comm(final)
    arrived(final % 2, 2 * blocks * kcs[0])
    start(w_down(0, 1 - final % 2))
    gather_ready(0, final)
    for n in range(blocks):
        gate = acc[n] + chunk_product(final, final % 2, n)
        up = acc[blocks + n] + chunk_product(final, final % 2, blocks + n)
        hid[:, n * WIDE : (n + 1) * WIDE] = gated(gate, up)
    base = CHUNKS[0]

    def full_tile(h, t, slot):
        r = jnp.dot(xv[h], ring[slot], preferred_element_type=F32)
        hid[:, pl.ds(pl.multiple_of(t * TILE, TILE), TILE)] = gated(r[:, :TILE], r[:, TILE:])

    def down_loop(h, base, lo):
        def trip(t, _):
            slot = (base + t) % 2
            u = lo + t
            stages(u, lo, at_start if h else once)
            if h == 0:
                when(t == 1, gather_diag, 1, 4)
                when(t < 3, gather_send, 1, 5 + t)
                when((t >= 2) & (t < 5), gather_relay, 1, 3 + t)
                when((t >= 4) & (t < 7), gather_diag, 1, 1 + t)
            arrived(slot, 2 * hidden)

            @pl.when(t + 1 < downs)
            def _():
                start(w_down(t + 1, 1 - slot))

            if h + 1 < HALVES:

                @pl.when(t + 1 == downs)
                def _():
                    start(w_full(0, 1 - slot))

            @pl.when(u >= SLOTS)
            def _():
                for b in range(2):
                    to_part(u - SLOTS, b).wait_send()
                    spend(free0.at[b], u)

            s, o = u % SLOTS, u % OWN
            for b in range(2):
                r = jnp.dot(hid[...], ring[slot, b * hidden : (b + 1) * hidden, :], preferred_element_type=F32)
                acc[o, pl.ds(b * group, group), :] = r[:group]
                send0[s, b] = r[group:].astype(BF16)
                if h:
                    to_part(u, b).start()
                    if b == 0:
                        stages(u, lo, at_middle)
            if not h:
                for b in range(2):
                    to_part(u, b).start()
            return 0

        lax.fori_loop(0, downs, trip, 0)

    down_loop(0, base, 0)
    base += downs

    def drain(c, _):
        gather_ready(1, c)
        return 0

    lax.fori_loop(0, CHUNKS[1], drain, 0)

    def full_trip(t, _):
        slot = (base + t) % 2
        stages(downs + t, 0, once)
        arrived(slot, depth)

        @pl.when(t + 1 < tiles)
        def _():
            start(w_full(t + 1, 1 - slot))

        @pl.when(t + 1 == tiles)
        def _():
            start(w_down(0, 1 - slot))

        full_tile(1, t, slot)
        return 0

    lax.fori_loop(0, tiles, full_trip, 0)
    down_loop(1, base + tiles, downs)

    def tail(v, _):
        stages(v, downs, at_start)
        stages(v, downs, at_middle)
        return 0

    lax.fori_loop(sums, sums + 3, tail, 0)

    for h in range(HALVES):

        def sent(c, _):
            gather_sent(h, c)
            return 0

        lax.fori_loop(0, CHUNKS[h], sent, 0)

    def last(u, _):
        for b in range(2):
            to_part(u, b).wait_send()
            for c in range(2):
                to_first(u, b, c).wait_send()
                to_second(u, b, c).wait_send()
        return 0

    lax.fori_loop(sums - SLOTS, sums, last, 0)
    for u in (sums - 2, sums - 1):
        for b in range(2):
            out_copy(u, b).wait()


def move(src, dst, buf, sem):
    n = sem.shape[1]
    rows = src.shape[0] // n
    at = [pl.ds(i * rows, rows) for i in range(n)]
    into = [pltpu.make_async_copy(src.at[at[i]], buf.at[at[i]], sem.at[0, i]) for i in range(n)]
    out = [pltpu.make_async_copy(buf.at[at[i]], dst.at[at[i]], sem.at[1, i]) for i in range(n)]
    for c in into:
        c.start()
    for i in range(n):
        into[i].wait()
        out[i].start()
    for c in out:
        c.wait()


def solution(mesh):
    def step(x, w_gate, w_up, w_down):
        n = mesh.shape["tp"]
        rows, depth = x.shape
        hidden = w_gate.shape[1]
        m = n * rows // HALVES
        r = rows // HALVES
        gathers = sum(CHUNKS)
        blocks = 2 * hidden // WIDE
        dma = pltpu.SemaphoreType.DMA
        y = pl.pallas_call(
            kernel,
            out_shape=jax.ShapeDtypeStruct((rows, depth), BF16),
            in_specs=[pl.BlockSpec(memory_space=pltpu.HBM)] * 4,
            out_specs=pl.BlockSpec(memory_space=pltpu.HBM),
            scratch_shapes=[
                pltpu.VMEM((HALVES, m, depth), BF16),
                pltpu.VMEM((m, hidden), BF16),
                pltpu.VMEM((2, depth, 2 * TILE), BF16),
                pltpu.VMEM((blocks, m, WIDE), F32),
                pltpu.VMEM((SLOTS, 2, 4 * r, WIDE), BF16),
                pltpu.VMEM((SLOTS, 2, 4 * r, WIDE), BF16),
                pltpu.VMEM((SLOTS, 2, 2, 2 * r, NARROW), BF16),
                pltpu.VMEM((SLOTS, 2, 2, 2 * r, NARROW), BF16),
                pltpu.VMEM((SLOTS, 2, 2, r, NARROW), BF16),
                pltpu.VMEM((SLOTS, 2, 2, r, NARROW), BF16),
                pltpu.VMEM((2, 2, r, WIDE), BF16),
                dma((2,)),
                dma((3,)),
                dma((2, 2)),
                dma((gathers, 8)),
                dma((gathers, 8)),
                dma((SLOTS, 2)),
                dma((SLOTS, 2)),
                dma((SLOTS, 2, 2)),
                dma((SLOTS, 2, 2)),
                dma((SLOTS, 2, 2)),
                dma((SLOTS, 2, 2)),
                pltpu.SemaphoreType.REGULAR((2,)),
                pltpu.SemaphoreType.REGULAR((2, 2)),
                pltpu.SemaphoreType.REGULAR((2, 2)),
            ],
            compiler_params=pltpu.CompilerParams(
                collective_id=0, has_side_effects=True, vmem_limit_bytes=67043328
            ),
        )(x, w_gate, w_up, w_down)
        return pl.pallas_call(
            move,
            out_shape=jax.ShapeDtypeStruct((rows, depth), BF16),
            in_specs=[pl.BlockSpec(memory_space=pltpu.HBM)],
            out_specs=pl.BlockSpec(memory_space=pltpu.HBM),
            scratch_shapes=[pltpu.VMEM((rows, depth), BF16), dma((2, MOVES))],
        )(y)

    return jax.shard_map(
        step,
        mesh=mesh,
        in_specs=(P(("dp", "tp"), None), P(None, "tp"), P(None, "tp"), P("tp", None)),
        out_specs=P(("dp", "tp"), None),
        check_vma=False,
    )
```
